8 devices in a mesh: sp: 8 (over z, y, x, core).
Axes of the slice: x: 2, y: 2, z: 1, core: 2. Of those that a mesh axis runs over, the one named last changes fastest.
Arguments:
- x: bfloat16 [8, 2048, 1536], P(None, 'sp')
- ln1_w: bfloat16 [1536], replicated
- w_qkv: bfloat16 [1536, 4608], replicated
- q_ln_w: bfloat16 [16, 96], replicated
- k_ln_w: bfloat16 [16, 96], replicated
- w_out: bfloat16 [1536, 1536], replicated
- grad_y: bfloat16 [8, 2048, 1536], P(None, 'sp')
Outputs:
- output 1: bfloat16 [8, 2048, 1536], P(None, 'sp')
- output 2: bfloat16 [8, 2048, 1536], P(None, 'sp')
- output 3: float32 [1536], replicated
- output 4: float32 [1536, 4608], replicated
- output 5: float32 [16, 96], replicated
- output 6: float32 [16, 96], replicated
- output 7: float32 [1536, 1536], replicated
All inputs are finite; a program needn't handle non-finite values.
Results may differ from the reference program's by a relative error of at most 0.0118169.
Values are sent between devices in bfloat16 or wider.
A program may use at most 1 GiB of HBM per device.

```python
import math
import jax
import jax.numpy as jnp
from jax import lax

BATCH_SIZE = 8
SEQ_LEN = 2048
D_MODEL = 1536
N_HEADS = 16
HEAD_DIM = 96
Q_BLOCK = math.gcd(SEQ_LEN, 256)


def alibi_slopes(n_heads):
    pow_two = 2 ** math.ceil(math.log2(n_heads))
    exponents = jnp.arange(1, pow_two + 1, dtype=jnp.float32) * (8.0 / pow_two)
    slopes = jnp.exp2(-exponents)
    if pow_two != n_heads:
        slopes = jnp.concatenate([slopes[1::2], slopes[0::2]])[:n_heads]
    return slopes


def layer_norm(values, weight):
    centered = values - jnp.mean(values, axis=-1, keepdims=True)
    var_val = jnp.mean(centered * centered, axis=-1, keepdims=True)
    return centered * lax.rsqrt(var_val + 1e-5) * weight


def bf_cast(values):
    return values.astype(jnp.bfloat16).astype(jnp.float32)


def setup_inputs(seed: int = 0) -> dict:
    key_list = jax.random.split(jax.random.key(seed), 8)
    act_shape = (BATCH_SIZE, SEQ_LEN, D_MODEL)
    w_scale = D_MODEL ** -0.5
    head_gain = jnp.exp2(jax.random.uniform(key_list[3], (N_HEADS, 1), jnp.float32, -1.0, 1.0))
    q_gain = (1.0 + 0.3 * jax.random.normal(key_list[4], (N_HEADS, HEAD_DIM), jnp.float32)) * head_gain
    return {
        'x': jax.random.normal(key_list[0], act_shape, jnp.float32).astype(jnp.bfloat16),
        'ln1_w': (1.0 + 0.3 * jax.random.normal(key_list[1], (D_MODEL,), jnp.float32)).astype(jnp.bfloat16),
        'w_qkv': (jax.random.normal(key_list[2], (D_MODEL, 3 * D_MODEL), jnp.float32) * w_scale).astype(jnp.bfloat16),
        'q_ln_w': q_gain.astype(jnp.bfloat16),
        'k_ln_w': (1.0 + 0.3 * jax.random.normal(key_list[5], (N_HEADS, HEAD_DIM), jnp.float32)).astype(jnp.bfloat16),
        'w_out': (jax.random.normal(key_list[6], (D_MODEL, D_MODEL), jnp.float32) * w_scale).astype(jnp.bfloat16),
        'grad_y': jax.random.normal(key_list[7], act_shape, jnp.float32).astype(jnp.bfloat16),
    }


def head_attention(head_args):
    q_head, k_head, v_head, head_slope = head_args
    key_pos = jnp.arange(SEQ_LEN)

    def block_attention(blk_idx):
        q_part = lax.dynamic_slice_in_dim(q_head, blk_idx * Q_BLOCK, Q_BLOCK, axis=1)
        scores = jnp.einsum('bqd,bkd->bqk', q_part, k_head) * (HEAD_DIM ** -0.5)
        pos_gap = (blk_idx * Q_BLOCK + jnp.arange(Q_BLOCK))[:, None] - key_pos[None, :]
        scores = jnp.where(pos_gap >= 0, scores - head_slope * pos_gap.astype(jnp.float32), -1e30)
        row_max = lax.stop_gradient(jnp.max(scores, axis=-1, keepdims=True))
        weights = jnp.exp(scores - row_max)
        weighted = jnp.einsum('bqk,bkd->bqd', weights, v_head)
        return weighted / jnp.sum(weights, axis=-1, keepdims=True)

    out_blocks = lax.map(jax.checkpoint(block_attention), jnp.arange(SEQ_LEN // Q_BLOCK))
    return jnp.moveaxis(out_blocks, 0, 1).reshape(BATCH_SIZE, SEQ_LEN, HEAD_DIM)


def forward_pass(x, ln1_w, w_qkv, q_ln_w, k_ln_w, w_out):
    h_act = bf_cast(layer_norm(x, ln1_w))
    qkv_raw = jnp.einsum('bsd,de->bse', h_act, w_qkv)
    q_all = bf_cast(layer_norm(qkv_raw[..., :D_MODEL], q_ln_w.reshape(D_MODEL)))
    k_all = bf_cast(layer_norm(qkv_raw[..., D_MODEL:2 * D_MODEL], k_ln_w.reshape(D_MODEL)))
    v_all = bf_cast(qkv_raw[..., 2 * D_MODEL:])
    head_shape = (BATCH_SIZE, SEQ_LEN, N_HEADS, HEAD_DIM)
    per_head = [jnp.moveaxis(tensor.reshape(head_shape), 2, 0) for tensor in (q_all, k_all, v_all)]
    o_heads = lax.map(jax.checkpoint(head_attention), (per_head[0], per_head[1], per_head[2], alibi_slopes(N_HEADS)))
    o_all = bf_cast(jnp.moveaxis(o_heads, 0, 2).reshape(BATCH_SIZE, SEQ_LEN, D_MODEL))
    return jnp.einsum('bsd,de->bse', o_all, w_out) + x


def reference(x, ln1_w, w_qkv, q_ln_w, k_ln_w, w_out, grad_y):
    y_val, pull_back = jax.vjp(forward_pass, x.astype(jnp.float32), ln1_w.astype(jnp.float32), w_qkv.astype(jnp.float32), q_ln_w.astype(jnp.float32), k_ln_w.astype(jnp.float32), w_out.astype(jnp.float32))
    grad_list = pull_back(grad_y.astype(jnp.float32))
    return (y_val.astype(jnp.bfloat16), grad_list[0].astype(jnp.bfloat16), grad_list[1], grad_list[2], grad_list[3], grad_list[4], grad_list[5])
```

```python
import math
import jax
import jax.numpy as jnp
import numpy as np
from jax import lax
from jax.experimental import pallas as pl
from jax.experimental.pallas import tpu as pltpu
from jax.sharding import PartitionSpec as P

F32 = jnp.float32
BF16 = jnp.bfloat16
LOG2E = 1.4426950408889634
PAD = 128
BLK = 512
CHUNKS = 4
SUM_STEPS = {0: [(0, ch) for ch in range(4)], 1: [(1, ch) for ch in range(4)], 4: [(2, 0)], 6: [(2, 1)], 7: [(2, 2)], 8: [(3, 0)],
             9: [(2, 3), (3, 1)], 10: [(4, 0)], 11: [(3, 2), (4, 1)], 12: [(3, 3)], 13: [(4, 2)], 14: [(4, 3)]}
BACK_STEPS = {0: [(0, ch) for ch in range(4)], 1: [(1, ch) for ch in range(4)], 3: [(2, 0)], 4: [(2, 1), (2, 2)], 5: [(2, 3), (3, 0)],
              6: [(3, 1), (3, 2), (4, 0)], 7: [(3, 3), (4, 1), (4, 2), (4, 3)]}
COLS = 512
TOK = 256


def alibi_slopes(n_heads):
    pow_two = 2 ** math.ceil(math.log2(n_heads))
    slopes = [2.0 ** (-8.0 * k / pow_two) for k in range(1, pow_two + 1)]
    if pow_two != n_heads:
        slopes = (slopes[1::2] + slopes[0::2])[:n_heads]
    return np.asarray(slopes, np.float64)


def slope_rows(n_heads, head_dim):
    raw = alibi_slopes(n_heads) * math.sqrt(head_dim)
    rows = np.zeros((n_heads, PAD - head_dim, 128), np.float32)
    rest = raw.copy()
    for part in range(3):
        cur = rest.astype(BF16).astype(np.float64)
        rows[:, part, :] = cur[:, None]
        rows[:, part + 3, :] = cur[:, None]
        rest = rest - cur
    return jnp.asarray(rows, BF16)


def key_bias_cols(seq_len, head_dim):
    pos = lax.broadcasted_iota(jnp.int32, (seq_len, PAD - head_dim), 0)
    col = lax.broadcasted_iota(jnp.int32, (seq_len, PAD - head_dim), 1)
    low = pos & 255
    val = jnp.where(col < 3, pos - low, jnp.where(col < 6, low, 0))
    return val.astype(F32).astype(BF16)


def causal_mask(values, fill):
    kpos = lax.broadcasted_iota(jnp.int32, values.shape, 0)
    qpos = lax.broadcasted_iota(jnp.int32, values.shape, 1)
    return jnp.where(kpos <= qpos, values, fill)


def fwd_kernel(q_ref, k_ref, v_ref, srow_ref, o_ref, lse_ref, k_sc, q_sc, s_sc):
    head_dim, seq_len = q_ref.shape
    coef = LOG2E / math.sqrt(head_dim)

    @pl.when(pl.program_id(0) == 0)
    def _():
        k_sc[:, head_dim:] = key_bias_cols(seq_len, head_dim)

    k_sc[:, :head_dim] = k_ref[...].T
    q_sc[:head_dim, :] = q_ref[...]
    for lane in range(0, seq_len, 128):
        q_sc[head_dim:, lane:lane + 128] = srow_ref[0]
    n_blk = seq_len // BLK
    for qb in range(n_blk):
        qs = slice(qb * BLK, (qb + 1) * BLK)
        buf = s_sc.at[qb % 2]
        row_max = None
        for kb in range(qb + 1):
            ks = slice(kb * BLK, (kb + 1) * BLK)
            raw = jnp.dot(k_sc[ks, :], q_sc[:, qs], preferred_element_type=F32)
            if kb == qb:
                raw = causal_mask(raw, -1e30)
            buf[ks, :] = raw
            cur = jnp.max(raw, axis=0, keepdims=True)
            row_max = cur if row_max is None else jnp.maximum(row_max, cur)
        shift = row_max * coef
        acc, row_sum = None, None
        for kb in range(qb + 1):
            ks = slice(kb * BLK, (kb + 1) * BLK)
            prob = jnp.exp2(buf[ks, :] * coef - shift)
            part = jnp.sum(prob, axis=0, keepdims=True)
            out = jnp.dot(v_ref[:, ks], prob.astype(BF16), preferred_element_type=F32)
            row_sum = part if row_sum is None else row_sum + part
            acc = out if acc is None else acc + out
        o_ref[:, qs] = (acc / row_sum).astype(BF16)
        lse_ref[0, :, qs] = shift + jnp.log2(row_sum)


def ride_along(g_ref, gsum_ref, sum_refs, steps, step):
    phases = sum_phases(g_ref, gsum_ref, *sum_refs)

    def advance(todo):
        for phase, ch in todo:
            phases[phase](ch)

    for at, todo in steps.items():
        @pl.when(step == at)
        def _():
            if at == 0:
                meet_all(lax.axis_index('sp'), lax.axis_size('sp'))
            advance(todo)
    return advance


def end_ride(advance, step):
    @pl.when(step == pl.num_programs(0) - 1)
    def _():
        advance([(phase, ch) for phase in (5, 6) for ch in range(CHUNKS)])


def bwd_kernel(q_ref, k_ref, v_ref, srow_ref, o_ref, do_ref, lse_ref, g_ref, dq_ref, dk_ref, dv_ref, gsum_ref,
               k_sc, q_sc, v_sc, qt_sc, dot_sc, p_sc, ds_sc, dq_sc, *sum_refs):
    step = pl.program_id(0)
    advance = ride_along(g_ref, gsum_ref, sum_refs, SUM_STEPS, step)
    head_dim, seq_len = q_ref.shape
    scale = head_dim ** -0.5
    coef = LOG2E * scale

    @pl.when(pl.program_id(0) == 0)
    def _():
        k_sc[:, head_dim:] = key_bias_cols(seq_len, head_dim)

    k_sc[:, :head_dim] = k_ref[...].T
    v_sc[...] = v_ref[...].T
    qt_sc[...] = q_ref[...].T
    dot_sc[...] = do_ref[...].T
    q_sc[:head_dim, :] = q_ref[...]
    for lane in range(0, seq_len, 128):
        q_sc[head_dim:, lane:lane + 128] = srow_ref[0]
    delta = jnp.sum(do_ref[...].astype(F32) * o_ref[...].astype(F32), axis=0, keepdims=True)
    lse = lse_ref[0]
    n_blk = seq_len // BLK
    for kb in range(n_blk):
        ks = slice(kb * BLK, (kb + 1) * BLK)
        for qb in range(kb, n_blk):
            qs = slice(qb * BLK, (qb + 1) * BLK)
            raw = jnp.dot(k_sc[ks, :], q_sc[:, qs], preferred_element_type=F32)
            prob = jnp.exp2(raw * coef - lse[:, qs])
            if qb == kb:
                prob = causal_mask(prob, 0.0)
            d_prob = jnp.dot(v_sc[ks, :], do_ref[:, qs], preferred_element_type=F32)
            d_s = (prob * (d_prob - delta[:, qs])).astype(BF16)
            p_sc[:, qs] = prob.astype(BF16)
            ds_sc[:, qs] = d_s
            d_q = jnp.dot(k_ref[:, ks], d_s, preferred_element_type=F32)
            if kb == 0:
                dq_sc[:, qs] = d_q
            else:
                dq_sc[:, qs] += d_q
        rest = slice(kb * BLK, seq_len)
        d_v = jnp.dot(p_sc[:, rest], dot_sc[rest, :], preferred_element_type=F32)
        d_k = jnp.dot(ds_sc[:, rest], qt_sc[rest, :], preferred_element_type=F32)
        dv_ref[:, ks] = d_v.T.astype(BF16)
        dk_ref[:, ks] = (d_k * scale).T.astype(BF16)
    dq_ref[...] = (dq_sc[...] * scale).astype(BF16)

    end_ride(advance, step)


def head_spec(head_dim, seq_len):
    return pl.BlockSpec((head_dim, seq_len), lambda h: (h, 0))


def attention_fwd(q_t, k_t, v_t, srows, n_heads):
    width, seq_len = q_t.shape
    head_dim = width // n_heads
    spec = head_spec(head_dim, seq_len)
    pairs = seq_len * seq_len // 2 * n_heads
    return pl.pallas_call(
        fwd_kernel,
        grid=(n_heads,),
        in_specs=[spec, spec, spec, pl.BlockSpec((1,) + srows.shape[1:], lambda h: (h, 0, 0))],
        out_specs=[spec, pl.BlockSpec((1, 1, seq_len), lambda h: (h, 0, 0))],
        out_shape=[jax.ShapeDtypeStruct((width, seq_len), BF16), jax.ShapeDtypeStruct((n_heads, 1, seq_len), F32)],
        scratch_shapes=[pltpu.VMEM((seq_len, PAD), BF16), pltpu.VMEM((PAD, seq_len), BF16), pltpu.VMEM((2, seq_len, BLK), F32)],
        compiler_params=pltpu.CompilerParams(dimension_semantics=('arbitrary',), vmem_limit_bytes=60 * 2 ** 20),
        cost_estimate=pl.CostEstimate(flops=pairs * 4 * 256, bytes_accessed=width * seq_len * 8, transcendentals=pairs),
        name='attn_fwd',
    )(q_t, k_t, v_t, srows)


def attention_bwd(q_t, k_t, v_t, srows, o_t, do_t, lse, n_heads, gwo):
    width, seq_len = q_t.shape
    head_dim = width // n_heads
    spec = head_spec(head_dim, seq_len)
    pairs = seq_len * seq_len // 2 * n_heads
    grad_shape = jax.ShapeDtypeStruct((width, seq_len), BF16)
    return pl.pallas_call(
        bwd_kernel,
        grid=(n_heads,),
        in_specs=[spec, spec, spec, pl.BlockSpec((1,) + srows.shape[1:], lambda h: (h, 0, 0)), spec, spec,
                  pl.BlockSpec((1, 1, seq_len), lambda h: (h, 0, 0)), pl.BlockSpec(memory_space=pl.ANY)],
        out_specs=[spec, spec, spec, pl.BlockSpec(memory_space=pl.ANY)],
        out_shape=[grad_shape, grad_shape, grad_shape, jax.ShapeDtypeStruct(sum_shape(gwo), F32)],
        scratch_shapes=[pltpu.VMEM((seq_len, PAD), BF16), pltpu.VMEM((PAD, seq_len), BF16), pltpu.VMEM((seq_len, head_dim), BF16),
                        pltpu.VMEM((seq_len, head_dim), BF16), pltpu.VMEM((seq_len, head_dim), BF16),
                        pltpu.VMEM((BLK, seq_len), BF16), pltpu.VMEM((BLK, seq_len), BF16), pltpu.VMEM((head_dim, seq_len), F32)]
                       + sum_scratch(*gwo.shape),
        compiler_params=pltpu.CompilerParams(dimension_semantics=('arbitrary',), collective_id=1, has_side_effects=True, vmem_limit_bytes=60 * 2 ** 20),
        cost_estimate=pl.CostEstimate(flops=pairs * 10 * 256, bytes_accessed=width * seq_len * 16, transcendentals=pairs),
        name='attn_bwd',
    )(q_t, k_t, v_t, srows, o_t, do_t, lse, gwo.reshape(sum_shape(gwo)))


def row_stats(values, axis):
    centered = values - jnp.mean(values, axis=axis, keepdims=True)
    rstd = lax.rsqrt(jnp.mean(centered * centered, axis=axis, keepdims=True) + 1e-5)
    return centered * rstd, rstd


def norm_grad(cot, unit, rstd, weight, axis):
    scaled = cot * weight
    mean_a = jnp.mean(scaled, axis=axis, keepdims=True)
    mean_b = jnp.mean(scaled * unit, axis=axis, keepdims=True)
    return rstd * (scaled - mean_a - unit * mean_b)


def wide(col_ref, width):
    return jnp.concatenate([col_ref[...]] * (width // 128), axis=1)


def xor_index(a, b):
    return sum(lax.rem(a // bit + b // bit, 2) * bit for bit in (1, 2, 4))


def proj_kernel(x_ref, ln1_ref, w_ref, qw_ref, kw_ref, ht_ref, q_ref, k_ref, v_ref, uq_ref, uk_ref, rq_ref, rk_ref, seq_ref,
                land, own_sem, send_sem, recv_sem):
    n_dev, _, d_model = land.shape
    step = pl.program_id(0)
    me = lax.axis_index('sp')

    def cp_block(hop):
        peer = xor_index(me, hop)
        return remote(x_ref.at[peer], land.at[hop], send_sem.at[hop], recv_sem.at[hop], peer)

    own = pltpu.make_async_copy(x_ref.at[me], land.at[0], own_sem)

    @pl.when(step == 0)
    def _():
        own.start()
        meet_all(me, n_dev)
        for hop in range(1, n_dev):
            cp_block(hop).start()
        own.wait()

    for hop in range(1, n_dev):
        @pl.when(step == hop)
        def _():
            cp_block(hop).wait()

    x_blk = land[step]
    seq_ref[...] = x_blk
    unit, _ = row_stats(x_blk.astype(F32), 1)
    h_act = (unit * ln1_ref[...]).astype(BF16)
    ht_ref[...] = h_act.T
    parts = ((0, q_ref, uq_ref, rq_ref, qw_ref), (d_model, k_ref, uk_ref, rk_ref, kw_ref))
    for base, out_ref, u_ref, r_ref, nw_ref in parts:
        raw = jnp.dot(h_act, w_ref[:, base:base + d_model], preferred_element_type=F32)
        unit, rstd = row_stats(raw, 1)
        unit = unit.T
        u_ref[...] = unit
        r_ref[...] = jnp.broadcast_to(rstd, (TOK, 128)).T[:1]
        out_ref[...] = (unit * wide(nw_ref, TOK)).astype(BF16)
    v_ref[...] = jnp.dot(h_act, w_ref[:, 2 * d_model:], preferred_element_type=F32).astype(BF16).T


def back_kernel(dq_ref, dk_ref, dv_ref, uq_ref, uk_ref, rq_ref, rk_ref, qw_ref, kw_ref, w_ref, x_ref, ln1_ref, gy_ref,
                g_ref, drq_ref, drk_ref, gx_ref, gqw_ref, gkw_ref, g1_ref, gsum_ref, d_sc, *sum_refs):
    d_model = x_ref.shape[1]
    step = pl.program_id(0)
    advance = ride_along(g_ref, gsum_ref, sum_refs, BACK_STEPS, step)

    @pl.when(step == 0)
    def _():
        gqw_ref[...] = jnp.zeros_like(gqw_ref)
        gkw_ref[...] = jnp.zeros_like(gkw_ref)
        g1_ref[...] = jnp.zeros_like(g1_ref)

    d_sc[2 * d_model:, :] = dv_ref[...]
    parts = ((0, dq_ref, uq_ref, rq_ref, qw_ref, drq_ref, gqw_ref), (d_model, dk_ref, uk_ref, rk_ref, kw_ref, drk_ref, gkw_ref))
    for base, d_ref, u_ref, r_ref, nw_ref, out_ref, gw_ref in parts:
        cot, unit = d_ref[...].astype(F32), u_ref[...]
        prod = cot * unit
        fold = prod[:, :128]
        for lane in range(128, TOK, 128):
            fold = fold + prod[:, lane:lane + 128]
        gw_ref[...] += fold
        d_raw = norm_grad(cot, unit, r_ref[...], wide(nw_ref, TOK), 0).astype(BF16)
        out_ref[...] = d_raw
        d_sc[base:base + d_model, :] = d_raw
    d_h = jnp.dot(w_ref[...], d_sc[...], preferred_element_type=F32)
    cot = d_h.astype(BF16).T.astype(F32)
    unit, rstd = row_stats(x_ref[...].astype(F32), 1)
    g1_ref[...] += jnp.sum(cot * unit, axis=0, keepdims=True)
    gx_ref[...] = (norm_grad(cot, unit, rstd, ln1_ref[...], 1) + gy_ref[...].astype(F32)).astype(BF16)
    end_ride(advance, step)


def token_specs(d_model):
    col = pl.BlockSpec((d_model, TOK), lambda t: (0, t))
    row = pl.BlockSpec((TOK, d_model), lambda t: (t, 0))
    stat = pl.BlockSpec((1, TOK), lambda t: (0, t))
    return col, row, stat


def whole(shape):
    return pl.BlockSpec(shape, lambda t: (0, 0), pipeline_mode=pl.Buffered(1))


def project(x, ln1_row, w_qkv, qw_col, kw_col):
    n_dev, _, d_model = x.shape
    seq_len = n_dev * TOK
    at = lambda t: xor_index(lax.axis_index('sp'), t)
    col = pl.BlockSpec((d_model, TOK), lambda t: (0, at(t)))
    stat = pl.BlockSpec((1, TOK), lambda t: (0, at(t)))
    act = jax.ShapeDtypeStruct((d_model, seq_len), BF16)
    act_f32 = jax.ShapeDtypeStruct((d_model, seq_len), F32)
    stat_f32 = jax.ShapeDtypeStruct((1, seq_len), F32)
    dma = pltpu.SemaphoreType.DMA
    return pl.pallas_call(
        proj_kernel,
        grid=(n_dev,),
        in_specs=[pl.BlockSpec(memory_space=pl.ANY), whole(ln1_row.shape), whole(w_qkv.shape), whole(qw_col.shape), whole(kw_col.shape)],
        out_specs=[col, col, col, col, col, col, stat, stat, pl.BlockSpec((TOK, d_model), lambda t: (at(t), 0))],
        out_shape=[act, act, act, act, act_f32, act_f32, stat_f32, stat_f32, jax.ShapeDtypeStruct((seq_len, d_model), BF16)],
        scratch_shapes=[pltpu.VMEM((n_dev, TOK, d_model), BF16), dma, dma((n_dev,)), dma((n_dev,))],
        compiler_params=pltpu.CompilerParams(dimension_semantics=('arbitrary',), collective_id=2, has_side_effects=True, vmem_limit_bytes=60 * 2 ** 20),
        cost_estimate=pl.CostEstimate(flops=6 * seq_len * d_model * d_model, bytes_accessed=40 * seq_len * d_model, transcendentals=0),
        name='project',
    )(x, ln1_row, w_qkv, qw_col, kw_col)


def back_project(dq_t, dk_t, dv_t, saved, qw_col, kw_col, w_qkv, x_seq, ln1_row, gy_seq, gwv):
    seq_len, d_model = x_seq.shape
    col, row, stat = token_specs(d_model)
    act = jax.ShapeDtypeStruct((d_model, seq_len), BF16)
    acc_spec = lambda shape: pl.BlockSpec(shape, lambda t: (0, 0), pipeline_mode=pl.Buffered(1))
    uq, uk, rq, rk = saved
    return pl.pallas_call(
        back_kernel,
        grid=(seq_len // TOK,),
        in_specs=[col, col, col, col, col, stat, stat, whole(qw_col.shape), whole(kw_col.shape), whole(w_qkv.shape), row, whole(ln1_row.shape), row, pl.BlockSpec(memory_space=pl.ANY)],
        out_specs=[col, col, row, acc_spec((d_model, 128)), acc_spec((d_model, 128)), acc_spec((1, d_model)), pl.BlockSpec(memory_space=pl.ANY)],
        out_shape=[act, act, jax.ShapeDtypeStruct((seq_len, d_model), BF16), jax.ShapeDtypeStruct((d_model, 128), F32),
                   jax.ShapeDtypeStruct((d_model, 128), F32), jax.ShapeDtypeStruct((1, d_model), F32), jax.ShapeDtypeStruct(sum_shape(gwv), F32)],
        scratch_shapes=[pltpu.VMEM((3 * d_model, TOK), BF16)] + sum_scratch(*gwv.shape),
        compiler_params=pltpu.CompilerParams(dimension_semantics=('arbitrary',), collective_id=3, has_side_effects=True, vmem_limit_bytes=67043328),
        cost_estimate=pl.CostEstimate(flops=6 * seq_len * d_model * d_model, bytes_accessed=40 * seq_len * d_model, transcendentals=0),
        name='back_project',
    )(dq_t, dk_t, dv_t, uq, uk, rq, rk, qw_col, kw_col, w_qkv, x_seq, ln1_row, gy_seq, gwv.reshape(sum_shape(gwv)))


def grad_kernel(*refs):
    h_ref, d_refs, out_ref = refs[0], refs[1:-1], refs[-1]
    steps = pl.num_programs(0) // len(d_refs)
    for part, d_ref in enumerate(d_refs):
        @pl.when(pl.program_id(0) // steps == part)
        def _():
            out_ref[...] = lax.dot_general(h_ref[...], d_ref[...], (((1,), (1,)), ((), ())), preferred_element_type=F32)


def weight_grad(h_t, parts):
    d_model, seq_len = h_t.shape
    steps = d_model // COLS
    col_map = lambda part: lambda i: (jnp.clip(i - part * steps, 0, steps - 1), 0)
    n_parts = len(parts)
    return pl.pallas_call(
        grad_kernel,
        grid=(n_parts * steps,),
        in_specs=[whole((d_model, seq_len))] + [pl.BlockSpec((COLS, seq_len), col_map(i)) for i in range(n_parts)],
        out_specs=pl.BlockSpec((d_model, COLS), lambda i: (0, i)),
        out_shape=jax.ShapeDtypeStruct((d_model, n_parts * d_model), F32),
        compiler_params=pltpu.CompilerParams(dimension_semantics=('arbitrary',), vmem_limit_bytes=60 * 2 ** 20),
        cost_estimate=pl.CostEstimate(flops=2 * n_parts * seq_len * d_model * d_model, bytes_accessed=8 * n_parts * d_model * d_model, transcendentals=0),
    )(h_t, *parts)


def sum_phases(g_ref, out_ref, acc, r0, r1, r2, loc_sem, p0_send, p0_recv, p1_send, p1_recv, p2_send, p2_recv,
               a2_send, a2_recv, a1_send, a1_recv, b1_send, b1_recv, ol_sem, or_send, or_recv):
    cols = acc.shape[-1]
    me = lax.axis_index('sp')
    core = lax.rem(me, 2)
    xb = lax.rem(me // 2, 2)
    yb = me // 4
    core_peer = me + 1 - 2 * core
    x_peer = me + 2 - 4 * xb
    y_peer = me + 4 - 8 * yb
    first, second = (xb, yb), (yb, xb)
    peer1, peer2 = (x_peer, y_peer), (y_peer, x_peer)

    def g1(ch, part):
        return r0.at[ch, part, 0]

    def g2(ch, part):
        return r0.at[ch, part, 1, 0]

    def span(ch):
        return pl.ds(pl.multiple_of(ch * cols, cols), cols)

    def cp_load(ch):
        return pltpu.make_async_copy(g_ref.at[core, :, :, :, :, span(ch)], acc.at[ch], loc_sem.at[ch])

    def cp_core(ch):
        return remote(g_ref.at[1 - core, :, :, :, :, span(ch)], r0.at[ch], p0_send.at[ch], p0_recv.at[ch], core_peer)

    def cp_first(ch, part):
        return remote(acc.at[ch, part, 1 - first[part]], r1.at[ch, part], p1_send.at[ch, part], p1_recv.at[ch, part], peer1[part])

    def cp_second(ch, part):
        return remote(r1.at[ch, part, 1 - second[part]], r2.at[ch, part], p2_send.at[ch, part], p2_recv.at[ch, part], peer2[part])

    def cp_back2(ch, part):
        return remote(r2.at[ch, part], g2(ch, part), a2_send.at[ch, part], a2_recv.at[ch, part], peer2[part])

    def cp_back1(ch, part):
        return remote(r2.at[ch, part], g1(ch, part).at[second[part]], a1_send.at[ch, part], a1_recv.at[ch, part], peer1[part])

    def cp_relay(ch, part):
        return remote(g2(ch, part), g1(ch, part).at[1 - second[part]], b1_send.at[ch, part], b1_recv.at[ch, part], peer1[part])

    def out_pair(ch, part, kind):
        if kind == 0:
            src, dst = r2.at[ch, part], out_ref.at[core, part, first[part], second[part], :, span(ch)]
        elif kind == 1:
            src, dst = g2(ch, part), out_ref.at[core, part, first[part], 1 - second[part], :, span(ch)]
        else:
            src, dst = g1(ch, part), out_ref.at[core, part, 1 - first[part], :, :, span(ch)]
        local = pltpu.make_async_copy(src, dst, ol_sem.at[ch, kind, part])
        return local, remote(src, dst, or_send.at[ch, kind, part], or_recv.at[ch, kind, part], core_peer)

    def start_out(ch, part, kind):
        for copy in out_pair(ch, part, kind):
            copy.start()

    def phase0(ch):
        cp_core(ch).start()
        cp_load(ch).start()

    def phase1(ch):
        cp_load(ch).wait()
        cp_core(ch).wait_recv()
        for part in range(2):
            for f in range(2):
                for s in range(2):
                    acc[ch, part, f, s] += r0[ch, part, f, s]
            cp_first(ch, part).start()

    def phase2(ch):
        for part in range(2):
            cp_first(ch, part).wait_recv()
            for s in range(2):
                r1[ch, part, s] += acc[ch, part, first[part], s]
            cp_second(ch, part).start()

    def phase3(ch):
        for part in range(2):
            cp_second(ch, part).wait_recv()
            r2[ch, part] += r1[ch, part, second[part]]
            cp_back2(ch, part).start()
            cp_back1(ch, part).start()
            start_out(ch, part, 0)

    def phase4(ch):
        for part in range(2):
            cp_back2(ch, part).wait_recv()
            cp_relay(ch, part).start()
            start_out(ch, part, 1)

    def phase5(ch):
        for part in range(2):
            cp_back1(ch, part).wait_recv()
            cp_relay(ch, part).wait_recv()
            start_out(ch, part, 2)

    def finish(ch):
        cp_core(ch).wait_send()
        for part in range(2):
            for make in (cp_first, cp_second, cp_back2, cp_back1, cp_relay):
                make(ch, part).wait_send()
            for kind in range(3):
                local, away = out_pair(ch, part, kind)
                local.wait()
                away.wait_send()
                away.wait_recv()

    return phase0, phase1, phase2, phase3, phase4, phase5, finish


def sum_scratch(rows, width):
    piece, cols = rows // 16, width // CHUNKS
    dma = pltpu.SemaphoreType.DMA
    buf = lambda *lead: pltpu.VMEM((CHUNKS,) + lead + (piece, cols), F32)
    return ([buf(2, 2, 2), buf(2, 2, 2), buf(2, 2), buf(2)] + [dma((CHUNKS,))] * 3 + [dma((CHUNKS, 2))] * 10
            + [dma((CHUNKS, 3, 2))] * 3)


def remote(src, dst, send, recv, peer):
    return pltpu.make_async_remote_copy(src_ref=src, dst_ref=dst, send_sem=send, recv_sem=recv, device_id=(peer,), device_id_type=pl.DeviceIdType.MESH)


def meet_all(me, n_dev):
    barrier = pltpu.get_barrier_semaphore()
    for hop in range(1, n_dev):
        pl.semaphore_signal(barrier, inc=1, device_id=(lax.rem(me + hop, n_dev),), device_id_type=pl.DeviceIdType.MESH)
    pl.semaphore_wait(barrier, n_dev - 1)


def reduce_kernel(g_ref, e_ref, out_ref, esum_ref, e_buf, e_send, e_recv, *sum_refs):
    me = lax.axis_index('sp')
    n_dev = e_buf.shape[0]
    meet_all(me, n_dev)
    phases = sum_phases(g_ref, out_ref, *sum_refs)

    def cp_small(hop, origin):
        return remote(e_ref, e_buf.at[origin], e_send.at[hop], e_recv.at[hop], lax.rem(me + hop, n_dev))

    for hop in range(1, n_dev):
        cp_small(hop, me).start()
    e_buf[me] = e_ref[...]
    for phase in phases:
        lax.fori_loop(0, CHUNKS, lambda ch, _: phase(ch), None)
    for hop in range(1, n_dev):
        cp_small(hop, lax.rem(me + n_dev - hop, n_dev)).wait()
    total = e_buf[0]
    for origin in range(1, n_dev):
        total = total + e_buf[origin]
    esum_ref[...] = total


def sum_shape(value):
    rows, width = value.shape
    return (2, 2, 2, 2, rows // 16, width)


def reduce_sum(value, small, n_dev):
    shape = sum_shape(value)
    dma = pltpu.SemaphoreType.DMA
    vmem = pl.BlockSpec(memory_space=pltpu.VMEM)
    out, small_sum = pl.pallas_call(
        reduce_kernel,
        in_specs=[pl.BlockSpec(memory_space=pl.ANY), vmem],
        out_specs=[pl.BlockSpec(memory_space=pl.ANY), vmem],
        out_shape=[jax.ShapeDtypeStruct(shape, F32), jax.ShapeDtypeStruct(small.shape, F32)],
        scratch_shapes=[pltpu.VMEM((n_dev,) + small.shape, F32), dma((n_dev,)), dma((n_dev,))] + sum_scratch(*value.shape),
        compiler_params=pltpu.CompilerParams(collective_id=0, has_side_effects=True, vmem_limit_bytes=60 * 2 ** 20),
        cost_estimate=pl.CostEstimate(flops=10 ** 9, bytes_accessed=8 * value.size, transcendentals=0),
        name='reduce_sum',
    )(value.reshape(shape), small)
    return out.reshape(value.shape), small_sum


def place_kernel(*refs):
    refs[-1][...] = refs[-2][...]


def place_columns(value, width, first, into=None):
    rows, cols = value.shape
    unit = min(cols, rows)
    step = rows // 6 if rows % 6 == 0 else rows // 4
    prior = [] if into is None else [into]
    return pl.pallas_call(
        place_kernel,
        grid=(rows // step, cols // unit),
        in_specs=[pl.BlockSpec(memory_space=pl.ANY)] * len(prior) + [pl.BlockSpec((step, unit), lambda i, j: (i, j))],
        out_specs=pl.BlockSpec((step, unit), lambda i, j: (i, j + first)),
        out_shape=jax.ShapeDtypeStruct((rows, width), value.dtype),
        input_output_aliases={0: 0} if prior else {},
        compiler_params=pltpu.CompilerParams(dimension_semantics=('arbitrary', 'arbitrary')),
        cost_estimate=pl.CostEstimate(flops=rows * cols, bytes_accessed=2 * rows * cols * value.dtype.itemsize, transcendentals=0),
        name='place_columns',
    )(*prior, value)


def dot(a, b, ca, cb):
    return lax.dot_general(a, b, (((ca,), (cb,)), ((), ())), preferred_element_type=F32)


def solution(mesh):
    seq_spec = P(None, 'sp', None)
    rep_spec = P()
    n_sp = mesh.shape['sp']

    def exchange(blocks):
        return lax.all_to_all(blocks, 'sp', 0, 0, tiled=True)

    def local_step(x, ln1_w, w_qkv, q_ln_w, k_ln_w, w_out, grad_y):
        n_batch, tok_loc, d_model = x.shape
        n_heads, head_dim = q_ln_w.shape
        seq_len = n_batch * tok_loc
        srows = slope_rows(n_heads, head_dim)
        ln1_row = ln1_w.astype(F32)[None]
        qw_col = jnp.broadcast_to(q_ln_w.reshape(d_model, 1).astype(F32), (d_model, 128))
        kw_col = jnp.broadcast_to(k_ln_w.reshape(d_model, 1).astype(F32), (d_model, 128))
        h_t, q_t, k_t, v_t, *saved, x_seq = project(x, ln1_row, w_qkv, qw_col, kw_col)
        x_seq, grad_y = lax.optimization_barrier((x_seq, grad_y))
        gy_seq = exchange(grad_y).reshape(seq_len, d_model)
        o_t, lse = attention_fwd(q_t, k_t, v_t, srows, n_heads)
        y_seq = (dot(o_t, w_out, 0, 0) + x_seq.astype(F32)).astype(BF16)
        y_seq, gy_seq = lax.optimization_barrier((y_seq, gy_seq))
        y = exchange(y_seq.reshape(x.shape))
        gwo_loc = dot(o_t, gy_seq, 1, 0)
        do_t = dot(w_out, gy_seq, 1, 1).astype(BF16)
        gwo_loc, do_t = lax.optimization_barrier((gwo_loc, do_t))
        dq_t, dk_t, dv_t, gwo_sum = attention_bwd(q_t, k_t, v_t, srows, o_t, do_t, lse, n_heads, gwo_loc)
        grad_w_out = gwo_sum.reshape(w_out.shape)
        gwv_loc = weight_grad(h_t, [dv_t])
        drq, drk, gx_seq, gqw, gkw, g1, gwv_sum = back_project(dq_t, dk_t, dv_t, saved, qw_col, kw_col, w_qkv, x_seq, ln1_row, gy_seq, gwv_loc)
        grad_w_v = gwv_sum.reshape(w_out.shape)
        y, gx_seq = lax.optimization_barrier((y, gx_seq))
        grad_x = exchange(gx_seq.reshape(x.shape))
        gwqk_loc = weight_grad(h_t, [drq, drk])
        y = place_columns(y.reshape(seq_len, d_model), d_model, 0).reshape(x.shape)
        grad_w_out = place_columns(grad_w_out, d_model, 0)
        partial = place_columns(grad_w_v, 3 * d_model, 2)
        small_loc = jnp.concatenate([g1, jnp.sum(gqw, axis=1)[None], jnp.sum(gkw, axis=1)[None], jnp.zeros((5, d_model), F32)], axis=0)
        y, grad_w_out, partial, gwqk_loc = lax.optimization_barrier((y, grad_w_out, partial, gwqk_loc))
        grad_w_qk, small = reduce_sum(gwqk_loc, small_loc, n_sp)
        grad_w_qkv = place_columns(grad_w_qk, 3 * d_model, 0, partial)
        return y, grad_x, small[0], grad_w_qkv, small[1].reshape(n_heads, head_dim), small[2].reshape(n_heads, head_dim), grad_w_out

    return jax.shard_map(local_step, mesh=mesh, in_specs=(seq_spec, rep_spec, rep_spec, rep_spec, rep_spec, rep_spec, seq_spec), out_specs=(seq_spec, seq_spec, rep_spec, rep_spec, rep_spec, rep_spec, rep_spec), check_vma=False)
```
